16 devices in a mesh: dp: 4 (over y, z, core), sp: 4 (over x).
Axes of the slice: x: 4, y: 2, z: 1, core: 2. Of those that a mesh axis runs over, the one named last changes fastest.
The devices are a block of a 4x4x4 slice.
Arguments:
- q: bfloat16 [128, 32, 160], P('dp'), parts along dimension 0
- k: bfloat16 [128, 4096, 8, 160], P('dp', 'sp'), parts along dimension 0
- v: bfloat16 [128, 4096, 8, 160], P('dp', 'sp'), parts along dimension 0
Outputs:
- q: bfloat16 [128, 32, 160], P('dp'), parts along dimension 0
There are 4 independent parts. The reference program is written for one: setup_inputs(seed, part) draws one part's arguments, and reference() takes and returns one part's arrays. A program takes and returns all parts, laid end to end along the dimension named above; each array names one.
All inputs are finite; a program needn't handle non-finite values.
Results may differ from the reference program's by a relative error of at most 0.012.
Values are sent between devices in bfloat16 or wider.
A program may use at most 1.5 GiB of HBM per device.

```python
import jax
import jax.numpy as jnp

BATCH = 32
CACHE = 4096
HEADS = 32
KV_HEADS = 8
HEAD = 160


def setup_inputs(seed: int = 0, part: int = 0) -> dict:
    kq, kk, kv = (jax.random.fold_in(k, part) for k in jax.random.split(jax.random.key(seed), 3))
    return {
        "q": (3 * jax.random.normal(kq, (BATCH, HEADS, HEAD), jnp.float32)).astype(jnp.bfloat16),
        "k": jax.random.normal(kk, (BATCH, CACHE, KV_HEADS, HEAD), jnp.float32).astype(jnp.bfloat16),
        "v": jax.random.normal(kv, (BATCH, CACHE, KV_HEADS, HEAD), jnp.float32).astype(jnp.bfloat16),
    }


def einsum(form, a, b):
    return jnp.einsum(form, a.astype(jnp.float32), b.astype(jnp.float32))


def reference(q, k, v):
    grouped = q.reshape(BATCH, KV_HEADS, -1, HEAD)
    scores = einsum("bgsd,bugd->bgsu", grouped, k) * HEAD**-0.5
    weights = jax.nn.softmax(scores, -1).astype(jnp.bfloat16)
    return einsum("bgsu,bugd->bgsd", weights, v).astype(jnp.bfloat16).reshape(BATCH, HEADS, HEAD)
```

```python
import functools

import jax
import jax.numpy as jnp
from jax import lax
from jax.experimental import pallas as pl
from jax.experimental.pallas import tpu as pltpu
from jax.sharding import PartitionSpec as P

F32, BF16 = jnp.float32, jnp.bfloat16
SLOTS = 4
LANES = 128
LOG2E = 1.4426950408889634


def kernel(axis, n, dims, q_hbm, k_hbm, v_hbm, out_hbm, q_ref, k_buf, v_buf, w_ref, acc_ref, row_ref, parts, stats, out_ref, q_sem, k_sem, v_sem, send_sem, recv_sem, stat_send, stat_recv, out_sem):
    batch, heads, kv_heads, head, run = dims
    share = heads // kv_heads
    pack = LANES // heads
    chunks = batch // pack
    me = lax.axis_index(axis)
    scale = head**-0.5 * LOG2E

    barrier = pltpu.get_barrier_semaphore()
    for step in range(1, n):
        pl.semaphore_signal(barrier, inc=1, device_id={axis: lax.rem(me + step, n)}, device_id_type=pl.DeviceIdType.MESH)

    def q_copy():
        return pltpu.make_async_copy(q_hbm, q_ref, q_sem)

    def k_copy(i):
        return pltpu.make_async_copy(k_hbm.at[i], k_buf.at[lax.rem(i, SLOTS)], k_sem.at[lax.rem(i, SLOTS)])

    def v_copy(i):
        return pltpu.make_async_copy(v_hbm.at[i], v_buf.at[lax.rem(i, SLOTS)], v_sem.at[lax.rem(i, SLOTS)])

    q_copy().start()
    for i in range(SLOTS):
        k_copy(i).start()
        v_copy(i).start()

    own = lax.broadcasted_iota(jnp.int32, (heads, kv_heads * head), 0) // share
    col = lax.broadcasted_iota(jnp.int32, (heads, kv_heads * head), 1)
    diagonal = (col >= own * head) & (col < own * head + head)

    def scores(i):
        q = q_ref[i]
        wide = jnp.where(diagonal, jnp.concatenate([q] * kv_heads, axis=1), jnp.zeros((), BF16))
        return jnp.dot(wide, k_buf[lax.rem(i, SLOTS)], preferred_element_type=F32)

    def weigh(i, s):
        place = lax.rem(i, pack) * heads
        s = s * scale
        high = jnp.max(s, axis=1, keepdims=True)
        weights = jnp.exp2(s - high)
        total = jnp.sum(weights, axis=1, keepdims=True)
        w_ref[pl.ds(pl.multiple_of(place, heads), heads), :] = weights.astype(BF16)
        lane = lax.broadcasted_iota(jnp.int32, (heads, LANES), 1)
        row = lax.broadcasted_iota(jnp.int32, (heads, LANES), 0)
        here = lane == row + place
        line = lax.broadcasted_iota(jnp.int32, (1, LANES), 1)
        mine = (line >= place) & (line < place + heads)
        slot = lax.rem(i // pack, 2)
        high = jnp.sum(jnp.where(here, high, 0.0), axis=0, keepdims=True)
        total = jnp.sum(jnp.where(here, total, 0.0), axis=0, keepdims=True)
        row_ref[slot, 0:1, :] = jnp.where(mine, high, row_ref[slot, 0:1, :])
        row_ref[slot, 1:2, :] = jnp.where(mine, total, row_ref[slot, 1:2, :])

    def values(i):
        place = lax.rem(i, pack) * heads
        seen = lax.dot_general(v_buf[lax.rem(i, SLOTS)], w_ref[...], (((1,), (1,)), ((), ())), preferred_element_type=F32)
        lane = lax.broadcasted_iota(jnp.int32, (head, LANES), 1)
        acc = acc_ref[...]
        for g in range(kv_heads):
            first = place + g * share
            acc = jnp.where((lane >= first) & (lane < first + share), seen[g * head : (g + 1) * head], acc)
        acc_ref[...] = acc

    def part_copy(c, step):
        peer = lax.rem(me + step, n)
        return pltpu.make_async_remote_copy(
            parts.at[me, c], parts.at[me, c], send_sem.at[c, step - 1], recv_sem.at[c, step - 1],
            device_id={axis: peer}, device_id_type=pl.DeviceIdType.MESH)

    def stat_copy(c, step):
        peer = lax.rem(me + step, n)
        return pltpu.make_async_remote_copy(
            stats.at[me, c], stats.at[me, c], stat_send.at[c, step - 1], stat_recv.at[c, step - 1],
            device_id={axis: peer}, device_id_type=pl.DeviceIdType.MESH)

    def send(c):
        stats[me, c] = row_ref[lax.rem(c, 2)]
        parts[me, c] = acc_ref[...].astype(BF16)
        for step in range(1, n):
            stat_copy(c, step).start()
            part_copy(c, step).start()

    def out_copy(c):
        rows = pl.ds(pl.multiple_of(c * LANES, LANES), LANES)
        return pltpu.make_async_copy(out_ref.at[rows], out_hbm.at[rows], out_sem.at[c])

    def combine(c):
        for step in range(1, n):
            stat_copy(c, step).wait_recv()
            part_copy(c, step).wait_recv()
        high = [stats[d, c, 0:1, :] for d in range(n)]
        top = functools.reduce(jnp.maximum, high)
        factor = [jnp.exp2(h - top) for h in high]
        total = sum(stats[d, c, 1:2, :] * factor[d] for d in range(n))
        seen = sum(parts[d, c].astype(F32) * factor[d] for d in range(n)) / total
        rows = pl.ds(pl.multiple_of(c * LANES, LANES), LANES)
        out_ref[rows, :] = seen.T.astype(BF16)
        out_copy(c).start()

    row_ref[...] = jnp.zeros_like(row_ref)
    acc_ref[...] = jnp.zeros_like(acc_ref)
    q_copy().wait()
    k_copy(0).wait()
    weigh(0, scores(0))
    k_copy(SLOTS).start()
    pl.semaphore_wait(barrier, n - 1)

    def body(i, carry):
        k_copy(i).wait()
        v_copy(i - 1).wait()
        s = scores(i)
        values(i - 1)
        weigh(i, s)

        @pl.when(i + SLOTS < batch)
        def _():
            k_copy(i + SLOTS).start()

        @pl.when(i - 1 + SLOTS < batch)
        def _():
            v_copy(i - 1 + SLOTS).start()

        @pl.when(lax.rem(i, pack) == 0)
        def _():
            send(i // pack - 1)

        @pl.when((lax.rem(i, pack) == pack - 1) & (i > pack))
        def _():
            combine(i // pack - 1)

        return carry

    lax.fori_loop(1, batch, body, 0)
    v_copy(batch - 1).wait()
    values(batch - 1)
    send(chunks - 1)
    combine(chunks - 1)

    def finish(c, carry):
        for step in range(1, n):
            stat_copy(c, step).wait_send()
            part_copy(c, step).wait_send()
        out_copy(c).wait()
        return carry

    lax.fori_loop(0, chunks, finish, 0)


def solution(mesh):
    axis = "sp"
    n = mesh.shape[axis]

    def step(q, k, v):
        batch, heads, head = q.shape
        run, kv_heads = k.shape[1], k.shape[2]
        flat = (batch, kv_heads * head, run)
        k = k.transpose(0, 2, 3, 1).reshape(flat)
        v = v.transpose(0, 2, 3, 1).reshape(flat)
        chunks = batch * heads // LANES
        out = pl.pallas_call(
            functools.partial(kernel, axis, n, (batch, heads, kv_heads, head, run)),
            out_shape=jax.ShapeDtypeStruct((batch * heads, head), BF16),
            in_specs=[pl.BlockSpec(memory_space=pl.ANY)] * 3,
            out_specs=pl.BlockSpec(memory_space=pl.ANY),
            scratch_shapes=[
                pltpu.VMEM((batch, heads, head), BF16),
                pltpu.VMEM((SLOTS,) + flat[1:], BF16),
                pltpu.VMEM((SLOTS,) + flat[1:], BF16),
                pltpu.VMEM((LANES, run), BF16),
                pltpu.VMEM((head, LANES), F32),
                pltpu.VMEM((2, 8, LANES), F32),
                pltpu.VMEM((n, chunks, head, LANES), BF16),
                pltpu.VMEM((n, chunks, 8, LANES), F32),
                pltpu.VMEM((batch * heads, head), BF16),
                pltpu.SemaphoreType.DMA,
                pltpu.SemaphoreType.DMA((SLOTS,)),
                pltpu.SemaphoreType.DMA((SLOTS,)),
                pltpu.SemaphoreType.DMA((chunks, n - 1)),
                pltpu.SemaphoreType.DMA((chunks, n - 1)),
                pltpu.SemaphoreType.DMA((chunks, n - 1)),
                pltpu.SemaphoreType.DMA((chunks, n - 1)),
                pltpu.SemaphoreType.DMA((chunks,)),
            ],
            compiler_params=pltpu.CompilerParams(collective_id=0, has_side_effects=True, vmem_limit_bytes=60 * 2**20),
        )(q, k, v)
        return out.reshape(q.shape)

    return jax.shard_map(
        step,
        mesh=mesh,
        in_specs=(P("dp", None, None), P("dp", "sp", None, None), P("dp", "sp", None, None)),
        out_specs=P("dp", None, None),
        check_vma=False,
    )
```

```python
import functools

import jax
import jax.numpy as jnp
from jax import lax
from jax.experimental import pallas as pl
from jax.experimental.pallas import tpu as pltpu
from jax.sharding import PartitionSpec as P

F32, BF16 = jnp.float32, jnp.bfloat16
SLOTS = 4
VMEM_LIMIT = 33554432
LANES = 128
LOG2E = 1.4426950408889634


def rem(a, b):
    return a % b if isinstance(a, int) else lax.rem(a, b)


def fold(x):
    groups = LANES // x.shape[1]
    rows = x.shape[0] // groups
    return jnp.concatenate([x[j * rows : (j + 1) * rows] for j in range(groups)], axis=1)


def unfold(x, lanes):
    return jnp.concatenate([x[:, j * lanes : (j + 1) * lanes] for j in range(LANES // lanes)], axis=0)


def kernel(axis, n, dims, q_hbm, k_hbm, v_hbm, out_ref, q_ref, wide_ref, k_buf, v_buf, w_ref, acc_ref, row_ref, parts, stats, last_parts, last_stats, q_sem, k_sem, v_sem, half_sem, send_sem, recv_sem, last_send, last_recv):
    batch, heads, kv_heads, head, run = dims
    share = heads // kv_heads
    rest = head - LANES
    pack = LANES // heads
    solo = pack - 1
    main = batch - solo
    chunks = batch // pack
    me = lax.axis_index(axis)
    scale = head**-0.5 * LOG2E
    steps = sorted(range(1, n), key=lambda step: min(step, n - step))

    barrier = pltpu.get_barrier_semaphore()
    for step in steps:
        pl.semaphore_signal(barrier, inc=1, device_id={axis: lax.rem(me + step, n)}, device_id_type=pl.DeviceIdType.MESH)

    def q_copy():
        return pltpu.make_async_copy(q_hbm, q_ref, q_sem)

    def k_copy(i):
        return pltpu.make_async_copy(k_hbm.at[i], k_buf.at[lax.rem(i, SLOTS)], k_sem.at[lax.rem(i, SLOTS)])

    def v_half(i, j):
        rows = pl.ds(j * (kv_heads // 2) * head, (kv_heads // 2) * head)
        return pltpu.make_async_copy(v_hbm.at[i, rows], v_buf.at[i % SLOTS, rows], half_sem.at[j])

    def v_copy(i):
        return pltpu.make_async_copy(v_hbm.at[i], v_buf.at[lax.rem(i, SLOTS)], v_sem.at[lax.rem(i, SLOTS)])

    q_copy().start()
    for i in range(SLOTS):
        k_copy(i).start()
        v_copy(i).start()

    own = lax.broadcasted_iota(jnp.int32, (heads, kv_heads * head), 0) // share
    col = lax.broadcasted_iota(jnp.int32, (heads, kv_heads * head), 1)
    diagonal = (col >= own * head) & (col < own * head + head)

    def place_of(i):
        return rem(i + pack - 1, pack) * heads

    def chunk_of(i):
        return (i + pack - 1) // pack

    def remote(ref, send, recv, key, step):
        return pltpu.make_async_remote_copy(
            ref.at[(me, *key)], ref.at[(me, *key)], send.at[(*key, step - 1)], recv.at[(*key, step - 1)],
            device_id={axis: lax.rem(me + step, n)}, device_id_type=pl.DeviceIdType.MESH)

    def part_copy(c, step):
        return remote(parts, send_sem.at[0], recv_sem.at[0], (c,), step)

    def stat_copy(c, step):
        return remote(stats, send_sem.at[1], recv_sem.at[1], (c,), step)

    def last_part_copy(i, step):
        return remote(last_parts, last_send.at[0], last_recv.at[0], (i - main,), step)

    def last_stat_copy(i, step):
        return remote(last_stats, last_send.at[1], last_recv.at[1], (i - main,), step)

    def widen(i):
        wide_ref[...] = jnp.where(diagonal, jnp.concatenate([q_ref[i]] * kv_heads, axis=1), jnp.zeros((), BF16))

    def scores(i):
        return jnp.dot(wide_ref[...], k_buf[rem(i, SLOTS)], preferred_element_type=F32)

    def lines(here, high, total):
        return [jnp.sum(jnp.where(here, x, 0.0), axis=0, keepdims=True) for x in (high, total)]

    def weigh(i, s):
        place = place_of(i)
        s = s * scale
        high = jnp.max(s, axis=1, keepdims=True)
        weights = jnp.exp2(s - high)
        total = jnp.sum(weights, axis=1, keepdims=True)
        w_ref[pl.ds(pl.multiple_of(place, heads), heads), :] = weights.astype(BF16)
        lane = lax.broadcasted_iota(jnp.int32, (heads, LANES), 1)
        row = lax.broadcasted_iota(jnp.int32, (heads, LANES), 0)
        if isinstance(i, int) and i >= main:
            high, total = lines(lane == row, high, total)
            last_stats[me, i - main, 0:1, :] = high
            last_stats[me, i - main, 1:2, :] = total
            for step in steps:
                last_stat_copy(i, step).start()
        else:
            high, total = lines(lane == row + place, high, total)
            line = lax.broadcasted_iota(jnp.int32, (1, LANES), 1)
            mine = (line >= place) & (line < place + heads)
            slot = rem(chunk_of(i), 2)
            row_ref[slot, 0:1, :] = jnp.where(mine, high, row_ref[slot, 0:1, :])
            row_ref[slot, 1:2, :] = jnp.where(mine, total, row_ref[slot, 1:2, :])

    tile = 256
    depths, spans = kv_heads * head // tile, 2
    wide_span = run // spans

    def score_piece(i, j, total):
        depth, span = j % depths, j // depths
        piece = jnp.dot(
            wide_ref[:, depth * tile : (depth + 1) * tile],
            k_buf[rem(i, SLOTS), depth * tile : (depth + 1) * tile, span * wide_span : (span + 1) * wide_span],
            preferred_element_type=F32)
        return piece if total is None else total + piece

    def value_piece(i, j):
        g, span = j // spans, j % spans
        across = slice(span * wide_span, (span + 1) * wide_span)
        return lax.dot_general(
            v_buf[rem(i, SLOTS), g * head : (g + 1) * head, across], w_ref[:, across], (((1,), (1,)), ((), ())), preferred_element_type=F32)

    def take(i, g, seen, acc):
        lane = lax.broadcasted_iota(jnp.int32, (head, LANES), 1)
        first = place_of(i) + g * share
        return jnp.where((lane >= first) & (lane < first + share), seen, acc)

    def keep(i, acc):
        if isinstance(i, int) and i >= main:
            place = place_of(i)
            rows = acc.T[place : place + heads]
            last_parts[me, i - main, :heads, :] = rows[:, :LANES].astype(BF16)
            last_parts[me, i - main, heads:, :] = fold(rows[:, LANES:]).astype(BF16)
            for step in steps:
                last_part_copy(i, step).start()
        else:
            acc_ref[...] = acc

    def values(i, arrive=()):
        acc = acc_ref[...]
        for g in range(kv_heads):
            if arrive and g == kv_heads // 2:
                arrive[0].wait()
            acc = take(i, g, sum(value_piece(i, g * spans + j) for j in range(spans)), acc)
        keep(i, acc)

    def both(i):
        acc, seen, total = acc_ref[...], None, [None] * spans
        for j in range(kv_heads * spans):
            piece = value_piece(i - 1, j)
            seen = piece if j % spans == 0 else seen + piece
            if j % spans == spans - 1:
                acc = take(i - 1, j // spans, seen, acc)
            if j < depths * spans:
                total[j // depths] = score_piece(i, j, total[j // depths])
        return jnp.concatenate(total, axis=1), acc

    def send(c):
        stats[me, c] = row_ref[rem(c, 2)]
        parts[me, c] = acc_ref[...].astype(BF16)
        for step in steps:
            stat_copy(c, step).start()
            part_copy(c, step).start()

    def factors(lines_of):
        high, total = [[lines_of(d)[j : j + 1] for d in range(n)] for j in range(2)]
        top = functools.reduce(jnp.maximum, high)
        factor = [jnp.exp2(h - top) for h in high]
        total = sum(t * f for t, f in zip(total, factor))
        return [f / total for f in factor]

    def combine(c):
        for step in steps:
            stat_copy(c, step).wait_recv()
            part_copy(c, step).wait_recv()
        factor = factors(lambda d: stats[d, c])
        seen = sum(parts[d, c].astype(F32) * factor[d] for d in range(n)).T.astype(BF16)
        if isinstance(c, int) and c == 0:
            out_ref[:heads, :] = seen[LANES - heads :]
        else:
            out_ref[pl.ds(pl.multiple_of((c * pack - solo) * heads, heads), LANES), :] = seen

    def combine_last(i):
        for step in steps:
            last_stat_copy(i, step).wait_recv()
        factor = factors(lambda d: last_stats[d, i - main])
        columns = jnp.concatenate(factor + [jnp.zeros((8 - n, LANES), F32)], axis=0).T[:heads]
        major = [jnp.broadcast_to(columns[:, d : d + 1], (heads, LANES)) for d in range(n)]
        minor = [fold(jnp.broadcast_to(columns[:, d : d + 1], (heads, rest))) for d in range(n)]
        for step in steps:
            last_part_copy(i, step).wait_recv()
        first = sum(last_parts[d, i - main, :heads, :].astype(F32) * major[d] for d in range(n))
        second = sum(last_parts[d, i - main, heads:, :].astype(F32) * minor[d] for d in range(n))
        out_ref[i * heads : (i + 1) * heads, :LANES] = first.astype(BF16)
        out_ref[i * heads : (i + 1) * heads, LANES:] = unfold(second, rest).astype(BF16)

    row_ref[...] = jnp.zeros_like(row_ref)
    acc_ref[...] = jnp.zeros_like(acc_ref)
    w_ref[...] = jnp.zeros_like(w_ref)
    q_copy().wait()
    widen(0)
    k_copy(0).wait()
    s = scores(0)
    widen(1)
    weigh(0, s)
    k_copy(SLOTS).start()
    pl.semaphore_wait(barrier, n - 1)

    def attend(i):
        k_copy(i).wait()
        v_copy(i - 1).wait()
        s, acc = both(i)
        widen(i + 1)
        weigh(i, s)
        keep(i - 1, acc)

    def body(i, carry):
        attend(i)

        @pl.when(i + SLOTS < batch)
        def _():
            v_copy(i - 1 + SLOTS).start()

        @pl.when(i + SLOTS == batch)
        def _():
            for j in range(2):
                v_half(batch - 1, j).start()

        @pl.when(i + SLOTS < batch)
        def _():
            k_copy(i + SLOTS).start()

        @pl.when(lax.rem(i, pack) == 1)
        def _():
            send(chunk_of(i - 1))

        @pl.when((lax.rem(i, pack) == 0) & (i > 2 * pack))
        def _():
            combine(i // pack - 2)

        return carry

    lax.fori_loop(1, main, body, 0)
    for i in range(main, batch):
        k_copy(i).wait()
        v_copy(i - 1).wait()
        s, acc = both(i)
        if i + 1 < batch:
            widen(i + 1)
        keep(i - 1, acc)
        weigh(i, s)
        if i == main:
            send(chunks - 1)
    v_half(batch - 1, 0).wait()
    values(batch - 1, [v_half(batch - 1, 1)])

    def finish(c, carry):
        for step in steps:
            stat_copy(c, step).wait_send()
            part_copy(c, step).wait_send()
        return carry

    lax.fori_loop(0, chunks, finish, 0)
    combine(0)
    combine(chunks - 2)
    combine(chunks - 1)
    for i in range(main, batch):
        for step in steps:
            last_stat_copy(i, step).wait_send()
            last_part_copy(i, step).wait_send()
        combine_last(i)


def solution(mesh):
    axis = "sp"
    n = mesh.shape[axis]

    def step(q, k, v):
        batch, heads, head = q.shape
        run, kv_heads = k.shape[1], k.shape[2]
        flat = (batch, kv_heads * head, run)
        q = pltpu.with_memory_space_constraint(q, pltpu.HBM)
        k = k.transpose(0, 2, 3, 1).reshape(flat)
        v = v.transpose(0, 2, 3, 1).reshape(flat)
        pack = LANES // heads
        chunks, solo = batch // pack, pack - 1
        out = pl.pallas_call(
            functools.partial(kernel, axis, n, (batch, heads, kv_heads, head, run)),
            out_shape=jax.ShapeDtypeStruct((batch * heads, head), BF16),
            in_specs=[pl.BlockSpec(memory_space=pl.ANY)] * 3,
            out_specs=pl.BlockSpec(memory_space=pltpu.VMEM),
            scratch_shapes=[
                pltpu.VMEM((batch, heads, head), BF16),
                pltpu.VMEM((heads, kv_heads * head), BF16),
                pltpu.VMEM((SLOTS,) + flat[1:], BF16),
                pltpu.VMEM((SLOTS,) + flat[1:], BF16),
                pltpu.VMEM((LANES, run), BF16),
                pltpu.VMEM((head, LANES), F32),
                pltpu.VMEM((2, 8, LANES), F32),
                pltpu.VMEM((n, chunks, head, LANES), BF16),
                pltpu.VMEM((n, chunks, 8, LANES), F32),
                pltpu.VMEM((n, solo, heads * head // LANES, LANES), BF16),
                pltpu.VMEM((n, solo, 8, LANES), F32),
                pltpu.SemaphoreType.DMA,
                pltpu.SemaphoreType.DMA((SLOTS,)),
                pltpu.SemaphoreType.DMA((SLOTS,)),
                pltpu.SemaphoreType.DMA((2,)),
                pltpu.SemaphoreType.DMA((2, chunks, n - 1)),
                pltpu.SemaphoreType.DMA((2, chunks, n - 1)),
                pltpu.SemaphoreType.DMA((2, solo, n - 1)),
                pltpu.SemaphoreType.DMA((2, solo, n - 1)),
            ],
            compiler_params=pltpu.CompilerParams(collective_id=0, has_side_effects=True, vmem_limit_bytes=VMEM_LIMIT),
        )(q, k, v)
        return out.reshape(q.shape)

    return jax.shard_map(
        step,
        mesh=mesh,
        in_specs=(P("dp", None, None), P("dp", "sp", None, None), P("dp", "sp", None, None)),
        out_specs=P("dp", None, None),
        check_vma=False,
    )
```

```python
import functools

import jax
import jax.numpy as jnp
from jax import lax
from jax.experimental import pallas as pl
from jax.experimental.pallas import tpu as pltpu
from jax.sharding import PartitionSpec as P

F32, BF16 = jnp.float32, jnp.bfloat16
SLOTS = 4
VMEM_LIMIT = 33554432
LANES = 128
LOG2E = 1.4426950408889634


def rem(a, b):
    return a % b if isinstance(a, int) else lax.rem(a, b)


def fold(x):
    groups = LANES // x.shape[1]
    rows = x.shape[0] // groups
    return jnp.concatenate([x[j * rows : (j + 1) * rows] for j in range(groups)], axis=1)


def unfold(x, lanes):
    return jnp.concatenate([x[:, j * lanes : (j + 1) * lanes] for j in range(LANES // lanes)], axis=0)


def kernel(axis, n, dims, q_hbm, k_hbm, v_hbm, out_ref, q_ref, wide_ref, k_buf, v_buf, w_ref, acc_ref, row_ref, parts, stats, last_parts, last_stats, q_sem, k_sem, v_sem, send_sem, recv_sem, last_send, last_recv):
    batch, heads, kv_heads, head, run = dims
    share = heads // kv_heads
    rest = head - LANES
    pack = LANES // heads
    solo = pack - 1
    main = batch - solo
    ahead = solo
    chunks = batch // pack
    me = lax.axis_index(axis)
    scale = head**-0.5 * LOG2E
    steps = sorted(range(1, n), key=lambda step: min(step, n - step))

    barrier = pltpu.get_barrier_semaphore()
    for step in steps:
        pl.semaphore_signal(barrier, inc=1, device_id={axis: lax.rem(me + step, n)}, device_id_type=pl.DeviceIdType.MESH)

    def q_copy():
        return pltpu.make_async_copy(q_hbm, q_ref, q_sem)

    def k_copy(i):
        return pltpu.make_async_copy(k_hbm.at[i], k_buf.at[lax.rem(i, SLOTS)], k_sem.at[lax.rem(i, SLOTS)])

    def v_copy(i):
        return pltpu.make_async_copy(v_hbm.at[i], v_buf.at[lax.rem(i, SLOTS)], v_sem.at[lax.rem(i, SLOTS)])

    q_copy().start()
    for i in range(ahead):
        k_copy(i).start()
    for i in range(SLOTS):
        v_copy(i).start()
        if i + ahead < SLOTS:
            k_copy(i + ahead).start()

    own = lax.broadcasted_iota(jnp.int32, (heads, kv_heads * head), 0) // share
    col = lax.broadcasted_iota(jnp.int32, (heads, kv_heads * head), 1)
    diagonal = (col >= own * head) & (col < own * head + head)

    def place_of(i):
        return rem(i + pack - 1, pack) * heads

    def chunk_of(i):
        return (i + pack - 1) // pack

    def remote(ref, send, recv, key, step):
        return pltpu.make_async_remote_copy(
            ref.at[(me, *key)], ref.at[(me, *key)], send.at[(*key, step - 1)], recv.at[(*key, step - 1)],
            device_id={axis: lax.rem(me + step, n)}, device_id_type=pl.DeviceIdType.MESH)

    def part_copy(c, step):
        return remote(parts, send_sem.at[0], recv_sem.at[0], (c,), step)

    def stat_copy(c, step):
        return remote(stats, send_sem.at[1], recv_sem.at[1], (c,), step)

    def last_part_copy(i, step):
        return remote(last_parts, last_send.at[0], last_recv.at[0], (i - main,), step)

    def last_stat_copy(i, step):
        return remote(last_stats, last_send.at[1], last_recv.at[1], (i - main,), step)

    def widen(i):
        wide_ref[...] = jnp.where(diagonal, jnp.concatenate([q_ref[i]] * kv_heads, axis=1), jnp.zeros((), BF16))

    def scores(i):
        return jnp.dot(wide_ref[...], k_buf[rem(i, SLOTS)], preferred_element_type=F32)

    def lines(here, high, total):
        return [jnp.sum(jnp.where(here, x, 0.0), axis=0, keepdims=True) for x in (high, total)]

    def weigh(i, s):
        place = place_of(i)
        s = s * scale
        high = jnp.max(s, axis=1, keepdims=True)
        weights = jnp.exp2(s - high)
        total = jnp.sum(weights, axis=1, keepdims=True)
        w_ref[pl.ds(pl.multiple_of(place, heads), heads), :] = weights.astype(BF16)
        lane = lax.broadcasted_iota(jnp.int32, (heads, LANES), 1)
        row = lax.broadcasted_iota(jnp.int32, (heads, LANES), 0)
        high, total = lines(lane == row + place, high, total)
        line = lax.broadcasted_iota(jnp.int32, (1, LANES), 1)
        mine = (line >= place) & (line < place + heads)
        slot = rem(chunk_of(i), 2)
        row_ref[slot, 0:1, :] = jnp.where(mine, high, row_ref[slot, 0:1, :])
        row_ref[slot, 1:2, :] = jnp.where(mine, total, row_ref[slot, 1:2, :])

    def tell_last(i):
        last_stats[me, i - main] = pltpu.roll(row_ref[rem(chunk_of(i), 2)], LANES - place_of(i), 1)
        for step in steps:
            last_stat_copy(i, step).start()

    tile = 256
    depths, spans = kv_heads * head // tile, 2
    wide_span = run // spans

    def score_piece(i, j, total):
        depth, span = j % depths, j // depths
        piece = jnp.dot(
            wide_ref[:, depth * tile : (depth + 1) * tile],
            k_buf[rem(i, SLOTS), depth * tile : (depth + 1) * tile, span * wide_span : (span + 1) * wide_span],
            preferred_element_type=F32)
        return piece if total is None else total + piece

    def value_piece(i, j):
        g, span = j // spans, j % spans
        across = slice(span * wide_span, (span + 1) * wide_span)
        return lax.dot_general(
            v_buf[rem(i, SLOTS), g * head : (g + 1) * head, across], w_ref[:, across], (((1,), (1,)), ((), ())), preferred_element_type=F32)

    def take(i, g, seen, acc):
        lane = lax.broadcasted_iota(jnp.int32, (head, LANES), 1)
        first = place_of(i) + g * share
        return jnp.where((lane >= first) & (lane < first + share), seen, acc)

    def pack_last(i, acc):
        rows = acc.T[place_of(i) : place_of(i) + heads]
        last_parts[me, i - main, :heads, :] = rows[:, :LANES].astype(BF16)
        last_parts[me, i - main, heads:, :] = fold(rows[:, LANES:]).astype(BF16)

    def send_last(i):
        for step in steps:
            last_part_copy(i, step).start()

    def pieces(acc, v=None, first=0, end=kv_heads, k=None):
        total, seen = [None] * spans, None
        for j in range(max((end - first) * spans if v is not None else 0, depths * spans if k is not None else 0)):
            g = first + j // spans
            if v is not None and g < end:
                piece = value_piece(v, g * spans + j % spans)
                seen = piece if j % spans == 0 else seen + piece
                if j % spans == spans - 1:
                    acc = take(v, g, seen, acc)
            if k is not None and j < depths * spans:
                total[j // depths] = score_piece(k, j, total[j // depths])
        return acc, (None if k is None else jnp.concatenate(total, axis=1))

    def send(c):
        stats[me, c] = row_ref[rem(c, 2)]
        parts[me, c] = acc_ref[...].astype(BF16)
        for step in steps:
            stat_copy(c, step).start()
            part_copy(c, step).start()

    def factors(lines_of):
        high, total = [[lines_of(d)[j : j + 1] for d in range(n)] for j in range(2)]
        top = functools.reduce(jnp.maximum, high)
        factor = [jnp.exp2(h - top) for h in high]
        total = sum(t * f for t, f in zip(total, factor))
        return [f / total for f in factor]

    def combine(c):
        for step in steps:
            stat_copy(c, step).wait_recv()
            part_copy(c, step).wait_recv()
        factor = factors(lambda d: stats[d, c])
        seen = sum(parts[d, c].astype(F32) * factor[d] for d in range(n)).T.astype(BF16)
        if isinstance(c, int) and c == 0:
            out_ref[:heads, :] = seen[LANES - heads :]
        else:
            out_ref[pl.ds(pl.multiple_of((c * pack - solo) * heads, heads), LANES), :] = seen

    def combine_last(i):
        for step in steps:
            last_stat_copy(i, step).wait_recv()
        factor = factors(lambda d: last_stats[d, i - main])
        columns = jnp.concatenate(factor + [jnp.zeros((8 - n, LANES), F32)], axis=0).T[:heads]
        major = [jnp.broadcast_to(columns[:, d : d + 1], (heads, LANES)) for d in range(n)]
        minor = [fold(jnp.broadcast_to(columns[:, d : d + 1], (heads, rest))) for d in range(n)]
        for step in steps:
            last_part_copy(i, step).wait_recv()
        first = sum(last_parts[d, i - main, :heads, :].astype(F32) * major[d] for d in range(n))
        second = sum(last_parts[d, i - main, heads:, :].astype(F32) * minor[d] for d in range(n))
        place = pl.ds(pl.multiple_of(i * heads, heads), heads)
        out_ref[place, :LANES] = first.astype(BF16)
        out_ref[place, LANES:] = unfold(second, rest).astype(BF16)

    row_ref[...] = jnp.zeros_like(row_ref)
    acc_ref[...] = jnp.zeros_like(acc_ref)
    w_ref[...] = jnp.zeros_like(w_ref)
    q_copy().wait()
    widen(0)
    for i in range(ahead):
        k_copy(i).wait()
        s = scores(i)
        widen(i + 1)
        weigh(i, s)
        k_copy(i + SLOTS).start()
    pl.semaphore_wait(barrier, n - 1)

    def body(i, carry):
        lead = i - 1 + ahead
        k_copy(lead).wait()
        v_copy(i - 1).wait()
        acc, s = pieces(acc_ref[...], v=i - 1, k=lead)
        widen(jnp.minimum(lead + 1, batch - 1))
        weigh(lead, s)
        acc_ref[...] = acc

        @pl.when(lead + SLOTS < batch)
        def _():
            k_copy(lead + SLOTS).start()

        @pl.when(i - 1 + SLOTS < batch)
        def _():
            v_copy(i - 1 + SLOTS).start()

        @pl.when(lead >= main)
        def _():
            tell_last(lead)

        @pl.when(lax.rem(i, pack) == 1)
        def _():
            send(chunk_of(i - 1))

        @pl.when((lax.rem(i, pack) == 0) & (i > 2 * pack))
        def _():
            combine(i // pack - 2)

        return carry

    lax.fori_loop(1, main + 1, body, 0)
    for i in range(main, batch):
        v_copy(i).wait()
        if i > main:
            pack_last(i - 1, acc_ref[...])
        acc, _ = pieces(acc_ref[...], v=i)
        if i > main:
            send_last(i - 1)
        acc_ref[...] = acc
    pack_last(batch - 1, acc)
    send_last(batch - 1)

    def finish(c, carry):
        for step in steps:
            stat_copy(c, step).wait_send()
            part_copy(c, step).wait_send()
        return carry

    lax.fori_loop(0, chunks, finish, 0)
    combine(0)
    combine(chunks - 2)
    combine(chunks - 1)

    def finish_last(i, carry):
        for step in steps:
            last_stat_copy(i, step).wait_send()
            last_part_copy(i, step).wait_send()
        combine_last(i)
        return carry

    lax.fori_loop(main, batch, finish_last, 0)


def solution(mesh):
    axis = "sp"
    n = mesh.shape[axis]

    def step(q, k, v):
        batch, heads, head = q.shape
        run, kv_heads = k.shape[1], k.shape[2]
        flat = (batch, kv_heads * head, run)
        q = pltpu.with_memory_space_constraint(q, pltpu.HBM)
        k = k.transpose(0, 2, 3, 1).reshape(flat)
        v = v.transpose(0, 2, 3, 1).reshape(flat)
        pack = LANES // heads
        chunks, solo = batch // pack, pack - 1
        out = pl.pallas_call(
            functools.partial(kernel, axis, n, (batch, heads, kv_heads, head, run)),
            out_shape=jax.ShapeDtypeStruct((batch * heads, head), BF16),
            in_specs=[pl.BlockSpec(memory_space=pl.ANY)] * 3,
            out_specs=pl.BlockSpec(memory_space=pltpu.VMEM),
            scratch_shapes=[
                pltpu.VMEM((batch, heads, head), BF16),
                pltpu.VMEM((heads, kv_heads * head), BF16),
                pltpu.VMEM((SLOTS,) + flat[1:], BF16),
                pltpu.VMEM((SLOTS,) + flat[1:], BF16),
                pltpu.VMEM((LANES, run), BF16),
                pltpu.VMEM((head, LANES), F32),
                pltpu.VMEM((2, 8, LANES), F32),
                pltpu.VMEM((n, chunks, head, LANES), BF16),
                pltpu.VMEM((n, chunks, 8, LANES), F32),
                pltpu.VMEM((n, solo, heads * head // LANES, LANES), BF16),
                pltpu.VMEM((n, solo, 8, LANES), F32),
                pltpu.SemaphoreType.DMA,
                pltpu.SemaphoreType.DMA((SLOTS,)),
                pltpu.SemaphoreType.DMA((SLOTS,)),
                pltpu.SemaphoreType.DMA((2, chunks, n - 1)),
                pltpu.SemaphoreType.DMA((2, chunks, n - 1)),
                pltpu.SemaphoreType.DMA((2, solo, n - 1)),
                pltpu.SemaphoreType.DMA((2, solo, n - 1)),
            ],
            compiler_params=pltpu.CompilerParams(collective_id=0, has_side_effects=True, vmem_limit_bytes=VMEM_LIMIT),
        )(q, k, v)
        return out.reshape(q.shape)

    return jax.shard_map(
        step,
        mesh=mesh,
        in_specs=(P("dp", None, None), P("dp", "sp", None, None), P("dp", "sp", None, None)),
        out_specs=P("dp", None, None),
        check_vma=False,
    )
```

```python
import functools

import jax
import jax.numpy as jnp
from jax import lax
from jax.experimental import pallas as pl
from jax.experimental.pallas import tpu as pltpu
from jax.sharding import PartitionSpec as P

F32, BF16 = jnp.float32, jnp.bfloat16
SLOTS = 4
VMEM_LIMIT = 33554432
LANES = 128
LOG2E = 1.4426950408889634


def rem(a, b):
    return a % b if isinstance(a, int) else lax.rem(a, b)


def fold(x):
    groups = LANES // x.shape[1]
    rows = x.shape[0] // groups
    return jnp.concatenate([x[j * rows : (j + 1) * rows] for j in range(groups)], axis=1)


def unfold(x, lanes):
    return jnp.concatenate([x[:, j * lanes : (j + 1) * lanes] for j in range(LANES // lanes)], axis=0)


def kernel(axis, n, dims, q_hbm, k_hbm, v_hbm, out_ref, q_ref, wide_ref, k_buf, v_buf, w_ref, acc_ref, row_ref, parts, stats, last_parts, last_stats, q_sem, k_sem, v_sem, send_sem, recv_sem, last_send, last_recv):
    batch, heads, kv_heads, head, run = dims
    share = heads // kv_heads
    rest = head - LANES
    pack = LANES // heads
    solo = pack - 1
    main = batch - solo
    ahead = solo
    chunks = batch // pack
    me = lax.axis_index(axis)
    scale = head**-0.5 * LOG2E
    steps = sorted(range(1, n), key=lambda step: min(step, n - step))

    barrier = pltpu.get_barrier_semaphore()
    for step in steps:
        pl.semaphore_signal(barrier, inc=1, device_id={axis: lax.rem(me + step, n)}, device_id_type=pl.DeviceIdType.MESH)

    def q_copy():
        return pltpu.make_async_copy(q_hbm, q_ref, q_sem)

    def k_copy(i):
        return pltpu.make_async_copy(k_hbm.at[i], k_buf.at[lax.rem(i, SLOTS)], k_sem.at[lax.rem(i, SLOTS)])

    def v_copy(i):
        return pltpu.make_async_copy(v_hbm.at[i], v_buf.at[lax.rem(i, SLOTS)], v_sem.at[lax.rem(i, SLOTS)])

    q_copy().start()
    for i in range(ahead):
        k_copy(i).start()
    for i in range(SLOTS):
        v_copy(i).start()
        if i + ahead < SLOTS:
            k_copy(i + ahead).start()

    own = lax.broadcasted_iota(jnp.int32, (heads, kv_heads * head), 0) // share
    col = lax.broadcasted_iota(jnp.int32, (heads, kv_heads * head), 1)
    diagonal = (col >= own * head) & (col < own * head + head)

    def place_of(i):
        return rem(i + pack - 1, pack) * heads

    def chunk_of(i):
        return (i + pack - 1) // pack

    def remote(ref, send, recv, key, step):
        return pltpu.make_async_remote_copy(
            ref.at[(me, *key)], ref.at[(me, *key)], send.at[(*key, step - 1)], recv.at[(*key, step - 1)],
            device_id={axis: lax.rem(me + step, n)}, device_id_type=pl.DeviceIdType.MESH)

    def part_copy(c, step):
        return remote(parts, send_sem.at[0], recv_sem.at[0], (c,), step)

    def stat_copy(c, step):
        return remote(stats, send_sem.at[1], recv_sem.at[1], (c,), step)

    def last_part_copy(i, step):
        return remote(last_parts, last_send.at[0], last_recv.at[0], (i - main,), step)

    def last_stat_copy(i, step):
        return remote(last_stats, last_send.at[1], last_recv.at[1], (i - main,), step)

    def widen(i):
        wide_ref[...] = jnp.where(diagonal, jnp.concatenate([q_ref[i]] * kv_heads, axis=1), jnp.zeros((), BF16))

    def scores(i):
        return jnp.dot(wide_ref[...], k_buf[rem(i, SLOTS)], preferred_element_type=F32)

    def lines(here, high, total):
        return [jnp.sum(jnp.where(here, x, 0.0), axis=0, keepdims=True) for x in (high, total)]

    def weigh(i, s):
        place = place_of(i)
        s = s * scale
        high = jnp.max(s, axis=1, keepdims=True)
        weights = jnp.exp2(s - high)
        total = jnp.sum(weights, axis=1, keepdims=True)
        w_ref[pl.ds(pl.multiple_of(place, heads), heads), :] = weights.astype(BF16)
        lane = lax.broadcasted_iota(jnp.int32, (heads, LANES), 1)
        row = lax.broadcasted_iota(jnp.int32, (heads, LANES), 0)
        high, total = lines(lane == row + place, high, total)
        line = lax.broadcasted_iota(jnp.int32, (1, LANES), 1)
        mine = (line >= place) & (line < place + heads)
        slot = rem(chunk_of(i), 2)
        row_ref[slot, 0:1, :] = jnp.where(mine, high, row_ref[slot, 0:1, :])
        row_ref[slot, 1:2, :] = jnp.where(mine, total, row_ref[slot, 1:2, :])

    def tell_last(i):
        last_stats[me, i - main] = pltpu.roll(row_ref[rem(chunk_of(i), 2)], LANES - place_of(i), 1)
        for step in steps:
            last_stat_copy(i, step).start()

    tile = 256
    depths, spans = kv_heads * head // tile, 2
    wide_span = run // spans

    def score_piece(i, j, total):
        depth, span = j % depths, j // depths
        piece = jnp.dot(
            wide_ref[:, depth * tile : (depth + 1) * tile],
            k_buf[rem(i, SLOTS), depth * tile : (depth + 1) * tile, span * wide_span : (span + 1) * wide_span],
            preferred_element_type=F32)
        return piece if total is None else total + piece

    def value_piece(i, j):
        g, span = j // spans, j % spans
        across = slice(span * wide_span, (span + 1) * wide_span)
        return lax.dot_general(
            v_buf[rem(i, SLOTS), g * head : (g + 1) * head, across], w_ref[:, across], (((1,), (1,)), ((), ())), preferred_element_type=F32)

    def take(i, g, seen, acc):
        lane = lax.broadcasted_iota(jnp.int32, (head, LANES), 1)
        first = place_of(i) + g * share
        return jnp.where((lane >= first) & (lane < first + share), seen, acc)

    def pack_last(i, acc):
        rows = acc.T[place_of(i) : place_of(i) + heads]
        last_parts[me, i - main, :heads, :] = rows[:, :LANES].astype(BF16)
        last_parts[me, i - main, heads:, :] = fold(rows[:, LANES:]).astype(BF16)

    def send_last(i):
        for step in steps:
            last_part_copy(i, step).start()

    def pieces(acc, v=None, first=0, end=kv_heads, k=None):
        total, seen = [None] * spans, None
        for j in range(max((end - first) * spans if v is not None else 0, depths * spans if k is not None else 0)):
            g = first + j // spans
            if v is not None and g < end:
                piece = value_piece(v, g * spans + j % spans)
                seen = piece if j % spans == 0 else seen + piece
                if j % spans == spans - 1:
                    acc = take(v, g, seen, acc)
            if k is not None and j < depths * spans:
                total[j // depths] = score_piece(k, j, total[j // depths])
        return acc, (None if k is None else jnp.concatenate(total, axis=1))

    def send(c):
        stats[me, c] = row_ref[rem(c, 2)]
        parts[me, c] = acc_ref[...].astype(BF16)
        for step in steps:
            stat_copy(c, step).start()
            part_copy(c, step).start()

    def factors(lines_of):
        high, total = [[lines_of(d)[j : j + 1] for d in range(n)] for j in range(2)]
        top = functools.reduce(jnp.maximum, high)
        factor = [jnp.exp2(h - top) for h in high]
        total = sum(t * f for t, f in zip(total, factor))
        return [f / total for f in factor]

    def combine(c):
        for step in steps:
            stat_copy(c, step).wait_recv()
            part_copy(c, step).wait_recv()
        factor = factors(lambda d: stats[d, c])
        seen = sum(parts[d, c].astype(F32) * factor[d] for d in range(n)).T.astype(BF16)
        if isinstance(c, int) and c == 0:
            out_ref[:heads, :] = seen[LANES - heads :]
        else:
            out_ref[pl.ds(pl.multiple_of((c * pack - solo) * heads, heads), LANES), :] = seen

    def combine_last(i):
        for step in steps:
            last_stat_copy(i, step).wait_recv()
        factor = factors(lambda d: last_stats[d, i - main])
        columns = jnp.concatenate(factor + [jnp.zeros((8 - n, LANES), F32)], axis=0).T[:heads]
        major = [jnp.broadcast_to(columns[:, d : d + 1], (heads, LANES)) for d in range(n)]
        minor = [fold(jnp.broadcast_to(columns[:, d : d + 1], (heads, rest))) for d in range(n)]
        for step in steps:
            last_part_copy(i, step).wait_recv()
        first = sum(last_parts[d, i - main, :heads, :].astype(F32) * major[d] for d in range(n))
        second = sum(last_parts[d, i - main, heads:, :].astype(F32) * minor[d] for d in range(n))
        place = pl.ds(pl.multiple_of(i * heads, heads), heads)
        out_ref[place, :LANES] = first.astype(BF16)
        out_ref[place, LANES:] = unfold(second, rest).astype(BF16)

    row_ref[...] = jnp.zeros_like(row_ref)
    acc_ref[...] = jnp.zeros_like(acc_ref)
    w_ref[...] = jnp.zeros_like(w_ref)
    q_copy().wait()
    widen(0)
    for i in range(ahead):
        k_copy(i).wait()
        s = scores(i)
        widen(i + 1)
        weigh(i, s)
        k_copy(i + SLOTS).start()
    pl.semaphore_wait(barrier, n - 1)

    def body(i, carry):
        lead = i - 1 + ahead
        k_copy(lead).wait()
        v_copy(i - 1).wait()
        acc, s = pieces(acc_ref[...], v=i - 1, k=lead)
        widen(jnp.minimum(lead + 1, batch - 1))
        weigh(lead, s)
        acc_ref[...] = acc

        @pl.when(lead + SLOTS < batch)
        def _():
            k_copy(lead + SLOTS).start()

        @pl.when(i - 1 + SLOTS < batch)
        def _():
            v_copy(i - 1 + SLOTS).start()

        @pl.when(lead >= main)
        def _():
            tell_last(lead)

        @pl.when(lax.rem(i, pack) == 1)
        def _():
            send(chunk_of(i - 1))

        @pl.when((lax.rem(i, pack) == 0) & (i > 2 * pack))
        def _():
            combine(i // pack - 2)

        return carry

    lax.fori_loop(1, main + 1, body, 0)
    for i in range(main, batch):
        if i != main + 1:
            v_copy(i).wait()
        if i == main:
            v_copy(i + 1).wait()
        if i > main:
            pack_last(i - 1, acc)
        acc, _ = pieces(acc_ref[...] if i == main else acc, v=i)
        if i == main + 1:
            send_last(i - 1)
    send_last(batch - 2)
    pack_last(batch - 1, acc)
    send_last(batch - 1)

    def finish(c, carry):
        for step in steps:
            stat_copy(c, step).wait_send()
            part_copy(c, step).wait_send()
        return carry

    lax.fori_loop(0, chunks, finish, 0)
    combine(0)
    combine(chunks - 2)
    combine(chunks - 1)

    def finish_last(i, carry):
        for step in steps:
            last_stat_copy(i, step).wait_send()
            last_part_copy(i, step).wait_send()
        combine_last(i)
        return carry

    lax.fori_loop(main, batch, finish_last, 0)


def solution(mesh):
    axis = "sp"
    n = mesh.shape[axis]

    def step(q, k, v):
        batch, heads, head = q.shape
        run, kv_heads = k.shape[1], k.shape[2]
        flat = (batch, kv_heads * head, run)
        q = pltpu.with_memory_space_constraint(q, pltpu.HBM)
        k = k.transpose(0, 2, 3, 1).reshape(flat)
        v = v.transpose(0, 2, 3, 1).reshape(flat)
        pack = LANES // heads
        chunks, solo = batch // pack, pack - 1
        out = pl.pallas_call(
            functools.partial(kernel, axis, n, (batch, heads, kv_heads, head, run)),
            out_shape=jax.ShapeDtypeStruct((batch * heads, head), BF16),
            in_specs=[pl.BlockSpec(memory_space=pl.ANY)] * 3,
            out_specs=pl.BlockSpec(memory_space=pltpu.VMEM),
            scratch_shapes=[
                pltpu.VMEM((batch, heads, head), BF16),
                pltpu.VMEM((heads, kv_heads * head), BF16),
                pltpu.VMEM((SLOTS,) + flat[1:], BF16),
                pltpu.VMEM((SLOTS,) + flat[1:], BF16),
                pltpu.VMEM((LANES, run), BF16),
                pltpu.VMEM((head, LANES), F32),
                pltpu.VMEM((2, 8, LANES), F32),
                pltpu.VMEM((n, chunks, head, LANES), BF16),
                pltpu.VMEM((n, chunks, 8, LANES), F32),
                pltpu.VMEM((n, solo, heads * head // LANES, LANES), BF16),
                pltpu.VMEM((n, solo, 8, LANES), F32),
                pltpu.SemaphoreType.DMA,
                pltpu.SemaphoreType.DMA((SLOTS,)),
                pltpu.SemaphoreType.DMA((SLOTS,)),
                pltpu.SemaphoreType.DMA((2, chunks, n - 1)),
                pltpu.SemaphoreType.DMA((2, chunks, n - 1)),
                pltpu.SemaphoreType.DMA((2, solo, n - 1)),
                pltpu.SemaphoreType.DMA((2, solo, n - 1)),
            ],
            compiler_params=pltpu.CompilerParams(collective_id=0, has_side_effects=True, vmem_limit_bytes=VMEM_LIMIT),
        )(q, k, v)
        return out.reshape(q.shape)

    return jax.shard_map(
        step,
        mesh=mesh,
        in_specs=(P("dp", None, None), P("dp", "sp", None, None), P("dp", "sp", None, None)),
        out_specs=P("dp", None, None),
        check_vma=False,
    )
```
